32 devices in a mesh: seq: 8 (over z, x), head: 4 (over y, core).
Axes of the slice: x: 2, y: 2, z: 4, core: 2. Of those that a mesh axis runs over, the one named last changes fastest.
Arguments:
- queries: float32 [16, 1024, 128], P('head', 'seq'), may hold values from -1.75 to 1.75
- keys: float32 [16, 1024, 128], P('head', 'seq'), may hold values from -1.75 to 1.75
- values: float32 [16, 1024, 128], P('head', 'seq'), may hold values from -10 to 10
- out_grad: float32 [16, 1024, 128], P('head', 'seq'), may hold values from -6 to 6
- norm_gain: float32 [16, 128], P('head'), may hold values from 0.1 to 1.9
- log_decay: float32 [16, 1024], P('head', 'seq'), may hold values from -1.5 to 0
- doc_ids: int32 [1024], P('seq'), may hold values from 0 to 7, never falling along the last dimension, each value on 1 to 512 neighbouring positions
Outputs:
- query_grad: float32 [16, 1024, 128], P('head', 'seq')
- key_grad: float32 [16, 1024, 128], P('head', 'seq')
- value_grad: float32 [16, 1024, 128], P('head', 'seq')
The draws below stay inside these ranges and needn't reach their ends.
Inputs may be any that keep to these rules, and one draw needn't show every extreme that they name: `doc_ids`: document numbers never fall along the tokens; each document is 1 to 512 consecutive tokens, and one has exactly 512.
All inputs are finite; a program needn't handle non-finite values.
Results may differ from the reference program's by a relative error of at most 0.0003.
Values sent between devices are 32-bit elements; how exact they have to be, the bound alone decides.
A program may use at most 64 MiB of HBM per device.

```python
import math
import jax
import jax.numpy as jnp
import numpy as np
from jax import lax

HEAD_DIM = 128
TOK_DEV = 128
HEADS = 16
PACKED_LENGTH = 1024
LONGEST_RECORD = 512
DOCS = 8


def draw_values(key, part):
    first_key, second_key = jax.random.split(jax.random.fold_in(key, 11))
    position = jnp.arange(HEADS, dtype=jnp.float32) / max(HEADS - 1, 1)
    entries = jax.random.truncated_normal(first_key, -4.0, 4.0, (HEADS, PACKED_LENGTH, HEAD_DIM), jnp.float32)
    rising = 0.5 * 4.0 ** position
    jitter = jax.random.uniform(second_key, (HEADS, 1, 1), jnp.float32, 0.8, 1.25)
    return entries * rising[:, None, None] * jitter


def draw_log_decay(key, part):
    base_key = jax.random.fold_in(key, 23)
    first_key, second_key, random_stream_c, fourth_key = jax.random.split(base_key, 4)
    fast_share = 0.4
    is_fast = jax.random.uniform(first_key, (HEADS, 1), jnp.float32) < fast_share
    slow_rate = 1.0 / LONGEST_RECORD
    fast_rate = 1.0 / min(40.0, TOK_DEV / 4.0)
    retention_multiplier = jnp.where(is_fast, fast_rate, slow_rate)
    attention_multiplier = jax.random.uniform(second_key, (HEADS, PACKED_LENGTH), jnp.float32, 0.5, 1.5)
    clustered_spans = jax.random.uniform(random_stream_c, (1, PACKED_LENGTH), jnp.float32) < 1.0 / LONGEST_RECORD
    objective_entries = jnp.log(jax.random.uniform(fourth_key, (1, PACKED_LENGTH), jnp.float32, 0.5, 0.8))
    return -retention_multiplier * attention_multiplier + jnp.where(clustered_spans, objective_entries, 0.0)


def level_of(key, dims, pieces, low, top_value):
    level, own = 1.0, jax.random.fold_in(key, 6)
    for dim, blocks in pieces:
        heights = jnp.exp(jax.random.uniform(jax.random.fold_in(own, dim), (blocks,), jnp.float32, low / len(pieces), top_value / len(pieces)))
        level = level * jnp.repeat(heights, dims[dim] // blocks).reshape([-1 if axis == dim else 1 for axis in range(len(dims))])
    return level


def profile(number_of, total, limit, lean):
    loads = [(1 << 20) // math.isqrt(rank ** lean) + 1 for rank in range(2, number_of + 1)]
    spare, counts = total - limit - (number_of - 1), [1] * (number_of - 1)
    while spare > 0:
        candidates = [i for i in range(number_of - 1) if counts[i] < limit]
        pool, remaining = sum([loads[i] for i in candidates]), spare
        for i in candidates:
            more = min(limit - counts[i], max(1, remaining * loads[i] // pool), spare)
            counts[i] = counts[i] + more
            spare = spare - more
    return np.array([limit] + counts)


def uneven_parts(rng, amount, total, reach, skew):
    if amount == 2:
        one = jax.random.randint(rng, (), max(1, total - reach), min(reach, total - 1) + 1)
        return jnp.stack([one, total - one])
    tallies = jnp.asarray(profile(amount, total, reach, skew), jnp.int32)
    twos = (amount - 1) // 2
    source_of, receiver = tallies[1:1 + 2 * twos:2], tallies[2:2 + 2 * twos:2]
    margin = jnp.minimum(source_of - 1, reach - receiver)
    shifted = jax.random.randint(jax.random.fold_in(rng, 1), (twos,), 0, 1 << 20) % (margin + 1)
    tallies = tallies.at[1:1 + 2 * twos:2].set(source_of - shifted).at[2:2 + 2 * twos:2].set(receiver + shifted)
    return tallies[jax.random.permutation(jax.random.fold_in(rng, 2), amount)]


def bell_draw(rng, dims, scale, bound, cuts=(), kind=jnp.bfloat16):
    values = jax.random.normal(rng, dims, jnp.float32) * scale
    if len(cuts) > 0:
        values = level_of(rng, dims, cuts, -0.22, 0.18) * values
    return jnp.clip(values, min=-bound, max=bound).astype(kind)


def setup_inputs(seed: int = 0) -> dict:
    seeds = jax.random.split(jax.random.key(seed), 8)
    return {
        "queries": bell_draw(seeds[0], (HEADS, PACKED_LENGTH, HEAD_DIM), (HEAD_DIM ** -0.25), 1.75, ((0, 4), (1, 8)), jnp.float32),
        "keys": bell_draw(seeds[1], (HEADS, PACKED_LENGTH, HEAD_DIM), (HEAD_DIM ** -0.25), 1.75, ((0, 4), (1, 8)), jnp.float32),
        "values": draw_values(jax.random.fold_in(seeds[7], 71), 0),
        "out_grad": bell_draw(seeds[3], (HEADS, PACKED_LENGTH, HEAD_DIM), 1.0, 6.0, ((0, 4), (1, 8)), jnp.float32),
        "norm_gain": jnp.clip(1.0 + 0.18 * jax.random.normal(seeds[4], (HEADS, HEAD_DIM), jnp.float32), 0.1, 1.9),
        "log_decay": draw_log_decay(jax.random.fold_in(seeds[7], 71), 0),
        "doc_ids": jnp.searchsorted(jnp.cumsum(uneven_parts(seeds[6], DOCS, PACKED_LENGTH, LONGEST_RECORD, 2)), jnp.arange(PACKED_LENGTH), side="right").astype(jnp.int32),
    }


EPSILON = 1e-06
PRECISE = lax.Precision.HIGHEST

def product(pattern, left_side, right_side):
    return jnp.einsum(pattern, left_side, right_side, precision=PRECISE, preferred_element_type=jnp.float32)

def block_weights(cumulative, labels):
    length = labels.shape[0]
    rows_iota = lax.broadcasted_iota(jnp.int32, (length, length), 0)
    cols_iota = lax.broadcasted_iota(jnp.int32, (length, length), 1)
    allowed = ((labels[:, None] == labels[None, :]) & (rows_iota >= cols_iota))[None]
    spread = cumulative[:, :, None] - cumulative[:, None, :]
    return jnp.where(allowed, jnp.exp(jnp.where(allowed, spread, 0.0)), 0.0)

def reference(queries, keys, values, out_grad, norm_gain, log_decay, doc_ids):
    queries = jnp.transpose(queries, (1, 0, 2))
    keys = jnp.transpose(keys, (1, 0, 2))
    values = jnp.transpose(values, (1, 0, 2))
    out_grad = jnp.transpose(out_grad, (1, 0, 2))
    blocks = PACKED_LENGTH // TOK_DEV
    query_blocks = queries.reshape(blocks, TOK_DEV, HEADS, HEAD_DIM)
    key_blocks = keys.reshape(blocks, TOK_DEV, HEADS, HEAD_DIM)
    value_blocks = values.reshape(blocks, TOK_DEV, HEADS, HEAD_DIM)
    decay_blocks = log_decay.reshape(HEADS, blocks, TOK_DEV).transpose(1, 0, 2)
    label_blocks = doc_ids.reshape(blocks, TOK_DEV)

    def forward_step(carried, inputs):
        prior_state, prior_label = carried
        block_queries, block_keys, block_values, block_decay, block_labels = inputs
        cumulative = jnp.cumsum(block_decay, axis=1)
        within = block_weights(cumulative, block_labels)
        scores = product('thd,shd->hts', block_queries, block_keys)
        from_prior = jnp.where((block_labels == prior_label)[:, None], jnp.exp(cumulative).T, 0.0)
        attended = product('hts,shd->thd', within * scores, block_values)
        attended = attended + from_prior[:, :, None] * product('thi,hij->thj', block_queries, prior_state)
        decay_tail = jnp.where((block_labels == block_labels[-1])[None, :], jnp.exp(cumulative[:, -1:] - cumulative), 0.0)
        kept_decay = jnp.where(block_labels[-1] == prior_label, jnp.exp(cumulative[:, -1]), 0.0)
        next_state = product('shi,shj->hij', block_keys * decay_tail.T[:, :, None], block_values)
        next_state = next_state + kept_decay[:, None, None] * prior_state
        return ((next_state, block_labels[-1]), (attended, prior_state))
    start_state = jnp.zeros((HEADS, HEAD_DIM, HEAD_DIM), jnp.float32)
    start_label = jnp.array(-1, jnp.int32)
    unused, (attended_blocks, prior_blocks) = lax.scan(forward_step, (start_state, start_label), (query_blocks, key_blocks, value_blocks, decay_blocks, label_blocks))
    attended = attended_blocks.reshape(PACKED_LENGTH, HEADS, HEAD_DIM)
    scaled_grad = norm_gain[None] * out_grad
    width_all = HEADS * HEAD_DIM
    inv_root = lax.rsqrt(lax.optimization_barrier(jnp.sum(attended * attended, axis=(1, 2))) / width_all + EPSILON)
    coupling = lax.optimization_barrier(jnp.sum(scaled_grad * attended, axis=(1, 2))) / width_all
    attn_grad = inv_root[:, None, None] * (scaled_grad - attended * (coupling * inv_root * inv_root)[:, None, None])
    grad_blocks = attn_grad.reshape(blocks, TOK_DEV, HEADS, HEAD_DIM)
    prior_labels = jnp.concatenate([jnp.array([-1], jnp.int32), label_blocks[:-1, -1]]).astype(jnp.int32)

    def grad_step(carried, inputs):
        later_state, later_label = carried
        block_queries, block_keys, block_values, block_grad, block_decay, block_labels, prior_state, prior_label = inputs
        cumulative = jnp.cumsum(block_decay, axis=1)
        within = block_weights(cumulative, block_labels)
        scores = product('thd,shd->hts', block_queries, block_keys)
        grad_weighted = within * product('thd,shd->hts', block_grad, block_values)
        from_prior = jnp.where((block_labels == prior_label)[:, None], jnp.exp(cumulative).T, 0.0)
        query_grad = product('hts,shd->thd', grad_weighted, block_keys)
        query_grad = query_grad + from_prior[:, :, None] * product('thj,hij->thi', block_grad, prior_state)
        to_next = jnp.where((block_labels == later_label)[:, None], jnp.exp(cumulative[:, -1:] - cumulative).T, 0.0)
        key_grad = product('hts,thd->shd', grad_weighted, block_queries)
        key_grad = key_grad + to_next[:, :, None] * product('hij,shj->shi', later_state, block_values)
        value_grad = product('hts,thd->shd', within * scores, block_grad)
        value_grad = value_grad + to_next[:, :, None] * product('hij,shi->shj', later_state, block_keys)
        from_start = jnp.where((block_labels == block_labels[0])[None, :], jnp.exp(cumulative), 0.0)
        kept_decay = jnp.where(block_labels[0] == later_label, jnp.exp(cumulative[:, -1]), 0.0)
        next_state = product('thi,thj->hij', block_queries * from_start.T[:, :, None], block_grad)
        next_state = next_state + kept_decay[:, None, None] * later_state
        return ((next_state, block_labels[0]), (query_grad, key_grad, value_grad))
    unused_two, (query_out, key_out, value_out) = lax.scan(grad_step, (start_state, start_label), (query_blocks, key_blocks, value_blocks, grad_blocks, decay_blocks, label_blocks, prior_blocks, prior_labels), reverse=True)
    return (jnp.transpose(query_out.reshape(PACKED_LENGTH, HEADS, HEAD_DIM), (1, 0, 2)), jnp.transpose(key_out.reshape(PACKED_LENGTH, HEADS, HEAD_DIM), (1, 0, 2)), jnp.transpose(value_out.reshape(PACKED_LENGTH, HEADS, HEAD_DIM), (1, 0, 2)))
```

```python
import functools
import jax
import jax.numpy as jnp
from jax import lax
from jax.experimental import pallas as pl
from jax.experimental.pallas import tpu as pltpu
from jax.sharding import PartitionSpec as P

EPSILON = 1e-06
F32 = jnp.float32
NN = (((1,), (0,)), ((), ()))
NT = (((1,), (1,)), ((), ()))
MESH = pl.DeviceIdType.MESH


def split(x):
    hi = x.astype(jnp.bfloat16)
    lo = (x - hi.astype(F32)).astype(jnp.bfloat16)
    return hi, lo


def mm(a, b, dims):
    def one(x, y):
        return lax.dot_general(x, y, dims, preferred_element_type=F32)

    return one(a[0], b[0]) + (one(a[0], b[1]) + one(a[1], b[0]))


def body(n, hs, q, k, v, og, gain, ld, doc, dq, dk, dv,
         own_f, pair_f, w_f, a_f, b_f, own_b, pair_b, w_b, a_b, b_b,
         att, wgt, wth, prior, ags, tot, send, recv, psend, precv):
    heads, rows, width = q.shape
    s = lax.axis_index("seq")
    hd = lax.axis_index("head")
    odd_i = lax.rem(s, 2)
    partner = s + 1 - 2 * odd_i
    odd = odd_i.astype(F32)
    even = 1.0 - odd
    has_up = s >= 2
    has_down = s < n - 2

    barrier = pltpu.get_barrier_semaphore()
    pl.semaphore_signal(barrier, inc=1, device_id={"seq": partner}, device_id_type=MESH)
    for j in range(1, hs):
        pl.semaphore_signal(barrier, inc=1, device_id={"head": lax.rem(hd + j, hs)}, device_id_type=MESH)

    @pl.when(has_up)
    def _():
        pl.semaphore_signal(barrier, inc=1, device_id={"seq": s - 2}, device_id_type=MESH)

    @pl.when(has_down)
    def _():
        pl.semaphore_signal(barrier, inc=1, device_id={"seq": s + 2}, device_id_type=MESH)

    def copy(kind, h, src, dst, to):
        return pltpu.make_async_remote_copy(
            src_ref=src.at[h], dst_ref=dst.at[h], send_sem=send.at[kind, h],
            recv_sem=recv.at[kind, h], device_id={"seq": to}, device_id_type=MESH)

    def x_f(h):
        return copy(0, h, own_f, pair_f, partner)

    def c_a(h):
        return copy(1, h, w_f, a_f, s + 2)

    def c_b(h):
        return copy(2, h, a_f, b_f, s + 2)

    def x_b(h):
        return copy(3, h, own_b, pair_b, partner)

    def d_a(h):
        return copy(4, h, w_b, a_b, s - 2)

    def d_b(h):
        return copy(5, h, a_b, b_b, s - 2)

    ri = lax.broadcasted_iota(jnp.int32, (rows, rows), 0)
    ci = lax.broadcasted_iota(jnp.int32, (rows, rows), 1)
    tri = jnp.where(ri <= ci, 1.0, 0.0)
    cum = lax.dot_general(ld[...], tri, NN, precision=lax.Precision.HIGHEST, preferred_element_type=F32)
    lab = doc[...].astype(F32) + 1.0
    first = jnp.broadcast_to(lab[:, 0:1], (1, width))
    last = jnp.broadcast_to(lab[:, rows - 1:rows], (1, width))
    mi = lax.broadcasted_iota(jnp.int32, (8, width), 0)

    def meta(passing, first_row, last_row):
        return jnp.where(mi == 0, passing, jnp.where(mi == 1, first_row, last_row))

    def parts(buf, h):
        return (buf[h, rows:rows + 1, :], buf[h, rows + 1:rows + 2, :], buf[h, rows + 2:rows + 3, :])

    def row(h):
        return cum[h:h + 1, :]

    def total(h):
        return cum[h:h + 1, rows - 1:rows]

    def passing(h):
        return jnp.broadcast_to(jnp.exp(total(h)), (1, width))

    def column(r):
        return jnp.broadcast_to(r, (width, r.shape[1])).T

    def put(buf, h, state):
        buf[h, 0:width, :] = state
        buf[h, width:width + 8, :] = meta(passing(h), first, last)

    for h in range(heads):
        tail = jnp.where(lab == last[:, 0:1], jnp.exp(total(h) - row(h)), 0.0)
        put(own_f, h, mm(split(k[h].T * tail), split(v[h]), NN))
        if h == 0:
            count = hs + has_up.astype(jnp.int32) + has_down.astype(jnp.int32)
            pl.semaphore_wait(barrier, count)
        x_f(h).start()

    @pl.when(s < 2)
    def _():
        a_f[...] = jnp.zeros_like(a_f)

    @pl.when(s < 4)
    def _():
        b_f[...] = jnp.zeros_like(b_f)

    @pl.when(s >= n - 2)
    def _():
        a_b[...] = jnp.zeros_like(a_b)

    @pl.when(s >= n - 4)
    def _():
        b_b[...] = jnp.zeros_like(b_b)

    lab_col = column(lab)
    allowed = (lab_col == lab) & (ri >= ci)

    def local_forward(h):
        spread = column(row(h)) - row(h)
        within = jnp.where(allowed, jnp.exp(jnp.where(allowed, spread, 0.0)), 0.0)
        wth[h] = within
        weighted = within * mm(split(q[h]), split(k[h]), NT)
        wgt[h] = weighted
        att[h] = mm(split(weighted), split(v[h]), NN)

    def merge_forward(h):
        x_f(h).wait_recv()
        p_pass, p_first, p_last = parts(pair_f, h)
        o_pass = passing(h)
        w_even = jnp.where((last == p_first) & (p_first == p_last), p_pass, 0.0)
        w_odd = jnp.where((p_last == first) & (first == last), o_pass, 0.0)
        c_own = odd + even * w_even
        c_pair = even + odd * w_odd
        w_f[h, 0:width, :] = c_own * own_f[h, 0:width, :] + c_pair * pair_f[h, 0:width, :]
        w_f[h, width:width + 8, :] = meta(
            o_pass * p_pass, even * first + odd * p_first, odd * last + even * p_last)

        @pl.when(has_down)
        def _():
            c_a(h).start()

    def relay_forward(h):
        @pl.when(has_up)
        def _():
            c_a(h).wait_recv()

        @pl.when(has_up & has_down)
        def _():
            c_b(h).start()

    def finish_forward(h):
        @pl.when(s >= 4)
        def _():
            c_b(h).wait_recv()

        a_pass, a_first, a_last = parts(a_f, h)
        b_last = parts(b_f, h)[2]
        p_pass, p_first, p_last = parts(pair_f, h)
        join = jnp.where((b_last == a_first) & (a_first == a_last), a_pass, 0.0)
        step = jnp.where((a_last == p_first) & (p_first == p_last), p_pass, 0.0)
        base = a_f[h, 0:width, :] + join * b_f[h, 0:width, :]
        state = (even + odd * step) * base + odd * pair_f[h, 0:width, :]
        prior[h] = state
        label = even * a_last + odd * p_last
        from_prior = column(jnp.where(lab == label, jnp.exp(row(h)), 0.0))
        attended = att[h] + from_prior * mm(split(q[h]), split(state), NN)
        att[h] = attended
        scaled = gain[h:h + 1, :] * og[h]
        return attended * attended, scaled * attended

    half = heads // 2
    for h in range(half):
        local_forward(h)
    for h in range(heads):
        merge_forward(h)
    for h in range(half, heads):
        local_forward(h)
    for h in range(heads):
        relay_forward(h)
    squares, inner = None, None
    for h in range(heads):
        one, two = finish_forward(h)
        squares = one if h == 0 else squares + one
        inner = two if h == 0 else inner + two
    sum_sq = jnp.sum(squares.T, axis=0, keepdims=True)
    sum_in = jnp.sum(inner.T, axis=0, keepdims=True)
    tot[0] = jnp.where(mi == 0, sum_sq, sum_in)

    def peer(j):
        return pltpu.make_async_remote_copy(
            src_ref=tot.at[0], dst_ref=tot.at[j], send_sem=psend.at[j], recv_sem=precv.at[j],
            device_id={"head": lax.rem(hd + j, hs)}, device_id_type=MESH)

    for j in range(1, hs):
        peer(j).start()
    for j in range(1, hs):
        peer(j).wait_recv()
    totals = tot[0]
    for j in range(1, hs):
        totals = totals + tot[j]
    width_all = heads * width * hs
    inv_row = lax.rsqrt(totals[0:1, :] / width_all + EPSILON)
    cpl_row = totals[1:2, :] / width_all * inv_row * inv_row
    inv_col = column(inv_row)
    cpl_col = column(cpl_row)

    for h in range(heads):
        grad = inv_col * (gain[h:h + 1, :] * og[h] - att[h] * cpl_col)
        ags[h] = grad
        from_start = jnp.where(lab == first[:, 0:1], jnp.exp(row(h)), 0.0)
        put(own_b, h, mm(split(q[h].T * from_start), split(grad), NN))
        x_b(h).start()

    def local_backward(h):
        grad = split(ags[h])
        gw = wth[h] * mm(grad, split(v[h]), NT)
        p_last = parts(pair_f, h)[2]
        label = even * parts(a_f, h)[2] + odd * p_last
        from_prior = column(jnp.where(lab == label, jnp.exp(row(h)), 0.0))
        dq[h] = mm(split(gw), split(k[h]), NN) + from_prior * mm(grad, split(prior[h]), NT)
        dk[h] = mm(split(gw.T), split(q[h]), NN)
        dv[h] = mm(split(wgt[h].T), grad, NN)

    def merge_backward(h):
        x_b(h).wait_recv()
        p_pass, p_first, p_last = parts(pair_b, h)
        o_pass = passing(h)
        w_even = jnp.where((last == p_first) & (first == last), o_pass, 0.0)
        w_odd = jnp.where((p_last == first) & (p_first == p_last), p_pass, 0.0)
        c_own = even + odd * w_odd
        c_pair = odd + even * w_even
        w_b[h, 0:width, :] = c_own * own_b[h, 0:width, :] + c_pair * pair_b[h, 0:width, :]
        w_b[h, width:width + 8, :] = meta(
            o_pass * p_pass, even * first + odd * p_first, odd * last + even * p_last)

        @pl.when(has_up)
        def _():
            d_a(h).start()

    def relay_backward(h):
        @pl.when(has_down)
        def _():
            d_a(h).wait_recv()

        @pl.when(has_up & has_down)
        def _():
            d_b(h).start()

    def finish_backward(h):
        @pl.when(s < n - 4)
        def _():
            d_b(h).wait_recv()

        a_pass, a_first, a_last = parts(a_b, h)
        b_first = parts(b_b, h)[1]
        p_pass, p_first, p_last = parts(pair_b, h)
        join = jnp.where((a_last == b_first) & (a_first == a_last), a_pass, 0.0)
        step = jnp.where((p_last == a_first) & (p_first == p_last), p_pass, 0.0)
        base = a_b[h, 0:width, :] + join * b_b[h, 0:width, :]
        state = split((odd + even * step) * base + even * pair_b[h, 0:width, :])
        label = odd * a_first + even * p_first
        to_next = column(jnp.where(lab == label, jnp.exp(total(h) - row(h)), 0.0))
        dk[h] = dk[h] + to_next * mm(split(v[h]), state, NT)
        dv[h] = dv[h] + to_next * mm(split(k[h]), state, NN)

    for h in range(half):
        local_backward(h)
    for h in range(heads):
        merge_backward(h)
    for h in range(half, heads):
        local_backward(h)
    for h in range(heads):
        relay_backward(h)
    for h in range(heads):
        finish_backward(h)

    for j in range(1, hs):
        peer(j).wait_send()
    for h in range(heads):
        x_f(h).wait_send()
        x_b(h).wait_send()

        @pl.when(has_down)
        def _():
            c_a(h).wait_send()

        @pl.when(has_up)
        def _():
            d_a(h).wait_send()

        @pl.when(has_up & has_down)
        def _():
            c_b(h).wait_send()
            d_b(h).wait_send()


def per_device(queries, keys, values, out_grad, norm_gain, log_decay, doc_ids):
    n, hs = lax.axis_size("seq"), lax.axis_size("head")
    heads, rows, width = queries.shape
    whole = pl.BlockSpec(memory_space=pltpu.VMEM)
    state = pltpu.VMEM((heads, width + 8, width), F32)
    square = pltpu.VMEM((heads, rows, width), F32)
    scores = pltpu.VMEM((heads, rows, rows), F32)
    out = jax.ShapeDtypeStruct(queries.shape, F32)
    return pl.pallas_call(
        functools.partial(body, n, hs),
        out_shape=(out, out, out),
        in_specs=[whole] * 7,
        out_specs=(whole, whole, whole),
        scratch_shapes=[state] * 10 + [
            square, scores, scores, pltpu.VMEM((heads, width, width), F32), square,
            pltpu.VMEM((hs, 8, rows), F32),
            pltpu.SemaphoreType.DMA((6, heads)), pltpu.SemaphoreType.DMA((6, heads)),
            pltpu.SemaphoreType.DMA((hs,)), pltpu.SemaphoreType.DMA((hs,)),
        ],
        compiler_params=pltpu.CompilerParams(
            collective_id=0, has_side_effects=True, vmem_limit_bytes=32 * 1024 * 1024),
    )(queries, keys, values, out_grad, norm_gain, log_decay, doc_ids[None, :])


def solution(mesh):
    in_specs = (
        P("head", "seq", None),
        P("head", "seq", None),
        P("head", "seq", None),
        P("head", "seq", None),
        P("head", None),
        P("head", "seq"),
        P("seq"),
    )
    out_specs = (P("head", "seq", None), P("head", "seq", None), P("head", "seq", None))
    return jax.shard_map(
        per_device, mesh=mesh, in_specs=in_specs, out_specs=out_specs, check_vma=False
    )
```

```python
import functools
import jax
import jax.numpy as jnp
from jax import lax
from jax.experimental import pallas as pl
from jax.experimental.pallas import tpu as pltpu
from jax.sharding import PartitionSpec as P

EPSILON = 1e-06
F32 = jnp.float32
NN = (((1,), (0,)), ((), ()))
NT = (((1,), (1,)), ((), ()))
MESH = pl.DeviceIdType.MESH


def split(x):
    hi = x.astype(jnp.bfloat16)
    lo = (x - hi.astype(F32)).astype(jnp.bfloat16)
    return hi, lo


def mm(a, b, dims):
    left = jnp.concatenate([a[0], a[1], a[0]], axis=1)
    right = jnp.concatenate([b[0], b[0], b[1]], axis=dims[0][1][0])
    return lax.dot_general(left, right, dims, preferred_element_type=F32)


def body(n, hs, q_in, k_in, v_in, og_in, gain_in, ld_in, doc_in, dq, dk, dv,
         q, k, v, og, gain, ld, doc, in_sem,
         own_f, pair_f, w_f, a_f, b_f, own_b, pair_b, w_b, a_b, b_b,
         att, wgt, wth, prior, ags, tot, send, recv, psend, precv):
    heads, rows, width = q.shape
    order = ((ld_in, ld), (doc_in, doc), (k_in, k), (v_in, v), (q_in, q), (og_in, og), (gain_in, gain))
    loads = [pltpu.make_async_copy(a, b, in_sem.at[i]) for i, (a, b) in enumerate(order)]
    for load in loads:
        load.start()
    s = lax.axis_index("seq")
    hd = lax.axis_index("head")
    odd_i = lax.rem(s, 2)
    partner = s + 1 - 2 * odd_i
    odd = odd_i.astype(F32)
    even = 1.0 - odd
    has_up = s >= 2
    has_down = s < n - 2

    barrier = pltpu.get_barrier_semaphore()
    pl.semaphore_signal(barrier, inc=1, device_id={"seq": partner}, device_id_type=MESH)
    for j in range(1, hs):
        pl.semaphore_signal(barrier, inc=1, device_id={"head": lax.rem(hd + j, hs)}, device_id_type=MESH)

    @pl.when(has_up)
    def _():
        pl.semaphore_signal(barrier, inc=1, device_id={"seq": s - 2}, device_id_type=MESH)

    @pl.when(has_down)
    def _():
        pl.semaphore_signal(barrier, inc=1, device_id={"seq": s + 2}, device_id_type=MESH)

    def copy(kind, h, src, dst, to):
        return pltpu.make_async_remote_copy(
            src_ref=src.at[h], dst_ref=dst.at[h], send_sem=send.at[kind, h],
            recv_sem=recv.at[kind, h], device_id={"seq": to}, device_id_type=MESH)

    def x_f(h):
        return copy(0, h, own_f, pair_f, partner)

    def c_a(h):
        return copy(1, h, w_f, a_f, s + 2)

    def c_b(h):
        return copy(2, h, a_f, b_f, s + 2)

    def x_b(h):
        return copy(3, h, own_b, pair_b, partner)

    def d_a(h):
        return copy(4, h, w_b, a_b, s - 2)

    def d_b(h):
        return copy(5, h, a_b, b_b, s - 2)

    loads[0].wait()
    loads[1].wait()
    ri = lax.broadcasted_iota(jnp.int32, (rows, rows), 0)
    ci = lax.broadcasted_iota(jnp.int32, (rows, rows), 1)
    tri = jnp.where(ri <= ci, 1.0, 0.0)
    cum = lax.dot_general(ld[...], tri, NN, precision=lax.Precision.HIGHEST, preferred_element_type=F32)
    lab = doc[...].astype(F32) + 1.0
    first = jnp.broadcast_to(lab[:, 0:1], (1, width))
    last = jnp.broadcast_to(lab[:, rows - 1:rows], (1, width))
    mi = lax.broadcasted_iota(jnp.int32, (8, width), 0)

    def meta(passing, first_row, last_row):
        return jnp.where(mi == 0, passing, jnp.where(mi == 1, first_row, last_row))

    def parts(buf, h):
        return (buf[h, rows:rows + 1, :], buf[h, rows + 1:rows + 2, :], buf[h, rows + 2:rows + 3, :])

    def row(h):
        return cum[h:h + 1, :]

    def total(h):
        return cum[h:h + 1, rows - 1:rows]

    def passing(h):
        return jnp.broadcast_to(jnp.exp(total(h)), (1, width))

    def column(r):
        return jnp.broadcast_to(r, (width, r.shape[1])).T

    def put(buf, h, state):
        buf[h, 0:width, :] = state
        buf[h, width:width + 8, :] = meta(passing(h), first, last)

    loads[2].wait()
    loads[3].wait()
    for h in range(heads):
        tail = jnp.where(lab == last[:, 0:1], jnp.exp(total(h) - row(h)), 0.0)
        put(own_f, h, mm(split(k[h].T * tail), split(v[h]), NN))
        if h == 0:
            count = hs + has_up.astype(jnp.int32) + has_down.astype(jnp.int32)
            pl.semaphore_wait(barrier, count)
        x_f(h).start()

    @pl.when(s < 2)
    def _():
        a_f[...] = jnp.zeros_like(a_f)

    @pl.when(s < 4)
    def _():
        b_f[...] = jnp.zeros_like(b_f)

    @pl.when(s >= n - 2)
    def _():
        a_b[...] = jnp.zeros_like(a_b)

    @pl.when(s >= n - 4)
    def _():
        b_b[...] = jnp.zeros_like(b_b)

    lab_col = column(lab)
    allowed = (lab_col == lab) & (ri >= ci)

    def local_forward(h):
        spread = column(row(h)) - row(h)
        within = jnp.where(allowed, jnp.exp(jnp.where(allowed, spread, 0.0)), 0.0)
        wth[h] = within
        weighted = within * mm(split(q[h]), split(k[h]), NT)
        wgt[h] = weighted
        att[h] = mm(split(weighted), split(v[h]), NN)

    def merge_forward(h):
        x_f(h).wait_recv()
        p_pass, p_first, p_last = parts(pair_f, h)
        o_pass = passing(h)
        w_even = jnp.where((last == p_first) & (p_first == p_last), p_pass, 0.0)
        w_odd = jnp.where((p_last == first) & (first == last), o_pass, 0.0)
        c_own = odd + even * w_even
        c_pair = even + odd * w_odd
        w_f[h, 0:width, :] = c_own * own_f[h, 0:width, :] + c_pair * pair_f[h, 0:width, :]
        w_f[h, width:width + 8, :] = meta(
            o_pass * p_pass, even * first + odd * p_first, odd * last + even * p_last)

        @pl.when(has_down)
        def _():
            c_a(h).start()

    def relay_forward(h):
        @pl.when(has_up)
        def _():
            c_a(h).wait_recv()

        @pl.when(has_up & has_down)
        def _():
            c_b(h).start()

    def finish_forward(h):
        @pl.when(s >= 4)
        def _():
            c_b(h).wait_recv()

        a_pass, a_first, a_last = parts(a_f, h)
        b_last = parts(b_f, h)[2]
        p_pass, p_first, p_last = parts(pair_f, h)
        join = jnp.where((b_last == a_first) & (a_first == a_last), a_pass, 0.0)
        step = jnp.where((a_last == p_first) & (p_first == p_last), p_pass, 0.0)
        base = a_f[h, 0:width, :] + join * b_f[h, 0:width, :]
        state = (even + odd * step) * base + odd * pair_f[h, 0:width, :]
        prior[h] = state
        label = even * a_last + odd * p_last
        from_prior = column(jnp.where(lab == label, jnp.exp(row(h)), 0.0))
        attended = att[h] + from_prior * mm(split(q[h]), split(state), NN)
        att[h] = attended
        scaled = gain[h:h + 1, :] * og[h]
        return attended * attended, scaled * attended

    half = heads // 2
    for load in loads[4:]:
        load.wait()
    for h in range(half):
        local_forward(h)
    for h in range(heads):
        merge_forward(h)
    for h in range(half, heads):
        local_forward(h)
    for h in range(heads):
        relay_forward(h)
    squares, inner = None, None
    for h in range(heads):
        one, two = finish_forward(h)
        squares = one if h == 0 else squares + one
        inner = two if h == 0 else inner + two
    sum_sq = jnp.sum(squares.T, axis=0, keepdims=True)
    sum_in = jnp.sum(inner.T, axis=0, keepdims=True)
    tot[0] = jnp.where(mi == 0, sum_sq, sum_in)

    def peer(j):
        return pltpu.make_async_remote_copy(
            src_ref=tot.at[0], dst_ref=tot.at[j], send_sem=psend.at[j], recv_sem=precv.at[j],
            device_id={"head": lax.rem(hd + j, hs)}, device_id_type=MESH)

    for j in range(1, hs):
        peer(j).start()
    for j in range(1, hs):
        peer(j).wait_recv()
    totals = tot[0]
    for j in range(1, hs):
        totals = totals + tot[j]
    width_all = heads * width * hs
    inv_row = lax.rsqrt(totals[0:1, :] / width_all + EPSILON)
    cpl_row = totals[1:2, :] / width_all * inv_row * inv_row
    inv_col = column(inv_row)
    cpl_col = column(cpl_row)

    for h in range(heads):
        grad = inv_col * (gain[h:h + 1, :] * og[h] - att[h] * cpl_col)
        ags[h] = grad
        from_start = jnp.where(lab == first[:, 0:1], jnp.exp(row(h)), 0.0)
        put(own_b, h, mm(split(q[h].T * from_start), split(grad), NN))
        x_b(h).start()

    def local_backward(h):
        grad = split(ags[h])
        gw = wth[h] * mm(grad, split(v[h]), NT)
        p_last = parts(pair_f, h)[2]
        label = even * parts(a_f, h)[2] + odd * p_last
        from_prior = column(jnp.where(lab == label, jnp.exp(row(h)), 0.0))
        dq[h] = mm(split(gw), split(k[h]), NN) + from_prior * mm(grad, split(prior[h]), NT)
        dk[h] = mm(split(gw.T), split(q[h]), NN)
        dv[h] = mm(split(wgt[h].T), grad, NN)

    def merge_backward(h):
        x_b(h).wait_recv()
        p_pass, p_first, p_last = parts(pair_b, h)
        o_pass = passing(h)
        w_even = jnp.where((last == p_first) & (first == last), o_pass, 0.0)
        w_odd = jnp.where((p_last == first) & (p_first == p_last), p_pass, 0.0)
        c_own = even + odd * w_odd
        c_pair = odd + even * w_even
        w_b[h, 0:width, :] = c_own * own_b[h, 0:width, :] + c_pair * pair_b[h, 0:width, :]
        w_b[h, width:width + 8, :] = meta(
            o_pass * p_pass, even * first + odd * p_first, odd * last + even * p_last)

        @pl.when(has_up)
        def _():
            d_a(h).start()

    def relay_backward(h):
        @pl.when(has_down)
        def _():
            d_a(h).wait_recv()

        @pl.when(has_up & has_down)
        def _():
            d_b(h).start()

    def finish_backward(h):
        @pl.when(s < n - 4)
        def _():
            d_b(h).wait_recv()

        a_pass, a_first, a_last = parts(a_b, h)
        b_first = parts(b_b, h)[1]
        p_pass, p_first, p_last = parts(pair_b, h)
        join = jnp.where((a_last == b_first) & (a_first == a_last), a_pass, 0.0)
        step = jnp.where((p_last == a_first) & (p_first == p_last), p_pass, 0.0)
        base = a_b[h, 0:width, :] + join * b_b[h, 0:width, :]
        state = split((odd + even * step) * base + even * pair_b[h, 0:width, :])
        label = odd * a_first + even * p_first
        to_next = column(jnp.where(lab == label, jnp.exp(total(h) - row(h)), 0.0))
        dk[h] = dk[h] + to_next * mm(split(v[h]), state, NT)
        dv[h] = dv[h] + to_next * mm(split(k[h]), state, NN)

    for h in range(half):
        local_backward(h)
    for h in range(heads):
        merge_backward(h)
    for h in range(half, heads):
        local_backward(h)
    for h in range(heads):
        relay_backward(h)
    for h in range(heads):
        finish_backward(h)

    for j in range(1, hs):
        peer(j).wait_send()
    for h in range(heads):
        x_f(h).wait_send()
        x_b(h).wait_send()

        @pl.when(has_down)
        def _():
            c_a(h).wait_send()

        @pl.when(has_up)
        def _():
            d_a(h).wait_send()

        @pl.when(has_up & has_down)
        def _():
            c_b(h).wait_send()
            d_b(h).wait_send()


def per_device(queries, keys, values, out_grad, norm_gain, log_decay, doc_ids):
    n, hs = lax.axis_size("seq"), lax.axis_size("head")
    heads, rows, width = queries.shape
    whole = pl.BlockSpec(memory_space=pltpu.VMEM)
    state = pltpu.VMEM((heads, width + 8, width), F32)
    square = pltpu.VMEM((heads, rows, width), F32)
    scores = pltpu.VMEM((heads, rows, rows), F32)
    out = jax.ShapeDtypeStruct(queries.shape, F32)
    return pl.pallas_call(
        functools.partial(body, n, hs),
        out_shape=(out, out, out),
        in_specs=[pl.BlockSpec(memory_space=pltpu.MemorySpace.HBM)] * 7,
        out_specs=(whole, whole, whole),
        scratch_shapes=[square] * 4 + [
            pltpu.VMEM(norm_gain.shape, F32), pltpu.VMEM(log_decay.shape, F32),
            pltpu.VMEM((1, rows), jnp.int32), pltpu.SemaphoreType.DMA((7,)),
        ] + [state] * 10 + [
            square, scores, scores, pltpu.VMEM((heads, width, width), F32), square,
            pltpu.VMEM((hs, 8, rows), F32),
            pltpu.SemaphoreType.DMA((6, heads)), pltpu.SemaphoreType.DMA((6, heads)),
            pltpu.SemaphoreType.DMA((hs,)), pltpu.SemaphoreType.DMA((hs,)),
        ],
        compiler_params=pltpu.CompilerParams(
            collective_id=0, has_side_effects=True, vmem_limit_bytes=32 * 1024 * 1024),
    )(queries, keys, values, out_grad, norm_gain, log_decay, doc_ids[None, :])


def solution(mesh):
    in_specs = (
        P("head", "seq", None),
        P("head", "seq", None),
        P("head", "seq", None),
        P("head", "seq", None),
        P("head", None),
        P("head", "seq"),
        P("seq"),
    )
    out_specs = (P("head", "seq", None), P("head", "seq", None), P("head", "seq", None))
    return jax.shard_map(
        per_device, mesh=mesh, in_specs=in_specs, out_specs=out_specs, check_vma=False
    )
```

```python
import functools
import jax
import jax.numpy as jnp
from jax import lax
from jax.experimental import pallas as pl
from jax.experimental.pallas import tpu as pltpu
from jax.sharding import PartitionSpec as P

EPSILON = 1e-06
F32 = jnp.float32
NN = (((1,), (0,)), ((), ()))
NT = (((1,), (1,)), ((), ()))
MESH = pl.DeviceIdType.MESH


def split(x):
    hi = x.astype(jnp.bfloat16)
    lo = (x - hi.astype(F32)).astype(jnp.bfloat16)
    return hi, lo


def mm(a, b, dims):
    left = jnp.concatenate([a[0], a[1], a[0]], axis=1)
    right = jnp.concatenate([b[0], b[0], b[1]], axis=dims[0][1][0])
    return lax.dot_general(left, right, dims, preferred_element_type=F32)


def body(n, hs, q_in, k_in, v_in, og_in, gain_in, ld_in, doc_in, dq, dk, dv,
         q, k, v, og, gain, ld, doc, in_sem,
         own_f, pair_f, w_f, a_f, b_f, own_b, pair_b, w_b, a_b, b_b,
         att, wgt, wth, prior, ags, tot, send, recv, psend, precv):
    heads, rows, width = q.shape
    order = ((ld_in, ld), (doc_in, doc), (k_in, k), (v_in, v), (q_in, q), (og_in, og), (gain_in, gain))
    loads = [pltpu.make_async_copy(a, b, in_sem.at[i]) for i, (a, b) in enumerate(order)]
    for load in loads:
        load.start()
    s = lax.axis_index("seq")
    hd = lax.axis_index("head")
    odd_i = lax.rem(s, 2)
    partner = s + 1 - 2 * odd_i
    odd = odd_i.astype(F32)
    even = 1.0 - odd
    has_up = s >= 2
    has_down = s < n - 2

    barrier = pltpu.get_barrier_semaphore()
    pl.semaphore_signal(barrier, inc=1, device_id={"seq": partner}, device_id_type=MESH)
    for j in range(1, hs):
        pl.semaphore_signal(barrier, inc=1, device_id={"head": lax.rem(hd + j, hs)}, device_id_type=MESH)

    @pl.when(has_up)
    def _():
        pl.semaphore_signal(barrier, inc=1, device_id={"seq": s - 2}, device_id_type=MESH)

    @pl.when(has_down)
    def _():
        pl.semaphore_signal(barrier, inc=1, device_id={"seq": s + 2}, device_id_type=MESH)

    def copy(kind, h, src, dst, to):
        return pltpu.make_async_remote_copy(
            src_ref=src.at[h], dst_ref=dst.at[h], send_sem=send.at[kind, h],
            recv_sem=recv.at[kind, h], device_id={"seq": to}, device_id_type=MESH)

    def x_f(h):
        return copy(0, h, own_f, pair_f, partner)

    def c_a(h):
        return copy(1, h, w_f, a_f, s + 2)

    def c_b(h):
        return copy(2, h, a_f, b_f, s + 2)

    def x_b(h):
        return copy(3, h, own_b, pair_b, partner)

    def d_a(h):
        return copy(4, h, w_b, a_b, s - 2)

    def d_b(h):
        return copy(5, h, a_b, b_b, s - 2)

    loads[0].wait()
    loads[1].wait()
    ri = lax.broadcasted_iota(jnp.int32, (rows, rows), 0)
    ci = lax.broadcasted_iota(jnp.int32, (rows, rows), 1)
    tri = jnp.where(ri <= ci, 1.0, 0.0)
    cum = lax.dot_general(ld[...], tri, NN, precision=lax.Precision.HIGHEST, preferred_element_type=F32)
    lab = doc[...].astype(F32) + 1.0
    first = jnp.broadcast_to(lab[:, 0:1], (1, width))
    last = jnp.broadcast_to(lab[:, rows - 1:rows], (1, width))
    mi = lax.broadcasted_iota(jnp.int32, (8, width), 0)

    def meta(passing, first_row, last_row):
        return jnp.where(mi == 0, passing, jnp.where(mi == 1, first_row, last_row))

    def parts(buf, h):
        return (buf[h, rows:rows + 1, :], buf[h, rows + 1:rows + 2, :], buf[h, rows + 2:rows + 3, :])

    def row(h):
        return cum[h:h + 1, :]

    def total(h):
        return cum[h:h + 1, rows - 1:rows]

    def passing(h):
        return jnp.broadcast_to(jnp.exp(total(h)), (1, width))

    def column(r):
        return jnp.broadcast_to(r, (width, r.shape[1])).T

    def put(buf, h, state):
        buf[h, 0:width, :] = state
        buf[h, width:width + 8, :] = meta(passing(h), first, last)

    loads[2].wait()
    loads[3].wait()
    for h in range(heads):
        tail = jnp.where(lab == last[:, 0:1], jnp.exp(total(h) - row(h)), 0.0)
        put(own_f, h, mm(split(k[h].T * tail), split(v[h]), NN))
        if h == 0:
            count = hs + has_up.astype(jnp.int32) + has_down.astype(jnp.int32)
            pl.semaphore_wait(barrier, count)
        x_f(h).start()

    @pl.when(s < 2)
    def _():
        a_f[...] = jnp.zeros_like(a_f)

    @pl.when(s < 4)
    def _():
        b_f[...] = jnp.zeros_like(b_f)

    @pl.when(s >= n - 2)
    def _():
        a_b[...] = jnp.zeros_like(a_b)

    @pl.when(s >= n - 4)
    def _():
        b_b[...] = jnp.zeros_like(b_b)

    lab_col = column(lab)
    allowed = (lab_col == lab) & (ri >= ci)

    def local_forward(h):
        spread = column(row(h)) - row(h)
        within = jnp.where(allowed, jnp.exp(jnp.where(allowed, spread, 0.0)), 0.0)
        wth[h] = within
        weighted = within * mm(split(q[h]), split(k[h]), NT)
        wgt[h] = weighted
        att[h] = mm(split(weighted), split(v[h]), NN)

    def merge_forward(h):
        x_f(h).wait_recv()
        p_pass, p_first, p_last = parts(pair_f, h)
        o_pass = passing(h)
        w_even = jnp.where((last == p_first) & (p_first == p_last), p_pass, 0.0)
        w_odd = jnp.where((p_last == first) & (first == last), o_pass, 0.0)
        c_own = odd + even * w_even
        c_pair = even + odd * w_odd
        w_f[h, 0:width, :] = c_own * own_f[h, 0:width, :] + c_pair * pair_f[h, 0:width, :]
        w_f[h, width:width + 8, :] = meta(
            o_pass * p_pass, even * first + odd * p_first, odd * last + even * p_last)

        @pl.when(has_down)
        def _():
            c_a(h).start()

    def relay_forward(h):
        @pl.when(has_up)
        def _():
            c_a(h).wait_recv()

        @pl.when(has_up & has_down)
        def _():
            c_b(h).start()

    def finish_forward(h):
        @pl.when(s >= 4)
        def _():
            c_b(h).wait_recv()

        a_pass, a_first, a_last = parts(a_f, h)
        b_last = parts(b_f, h)[2]
        p_pass, p_first, p_last = parts(pair_f, h)
        join = jnp.where((b_last == a_first) & (a_first == a_last), a_pass, 0.0)
        step = jnp.where((a_last == p_first) & (p_first == p_last), p_pass, 0.0)
        base = a_f[h, 0:width, :] + join * b_f[h, 0:width, :]
        state = (even + odd * step) * base + odd * pair_f[h, 0:width, :]
        prior[h] = state
        label = even * a_last + odd * p_last
        from_prior = column(jnp.where(lab == label, jnp.exp(row(h)), 0.0))
        attended = att[h] + from_prior * mm(split(q[h]), split(state), NN)
        att[h] = attended
        scaled = gain[h:h + 1, :] * og[h]
        return attended * attended, scaled * attended

    half = heads // 2
    for load in loads[4:]:
        load.wait()
    for h in range(half):
        local_forward(h)
    for h in range(heads):
        merge_forward(h)
    for h in range(half, heads):
        local_forward(h)
    for h in range(heads):
        relay_forward(h)
    squares, inner = None, None
    for h in range(heads):
        one, two = finish_forward(h)
        squares = one if h == 0 else squares + one
        inner = two if h == 0 else inner + two
    sum_sq = jnp.sum(squares.T, axis=0, keepdims=True)
    sum_in = jnp.sum(inner.T, axis=0, keepdims=True)
    tot[0] = jnp.where(mi == 0, sum_sq, sum_in)

    def peer(j):
        return pltpu.make_async_remote_copy(
            src_ref=tot.at[0], dst_ref=tot.at[j], send_sem=psend.at[j], recv_sem=precv.at[j],
            device_id={"head": lax.rem(hd + j, hs)}, device_id_type=MESH)

    for j in range(1, hs):
        peer(j).start()
    for j in range(1, hs):
        peer(j).wait_recv()
    totals = tot[0]
    for j in range(1, hs):
        totals = totals + tot[j]
    width_all = heads * width * hs
    inv_row = lax.rsqrt(totals[0:1, :] / width_all + EPSILON)
    cpl_row = totals[1:2, :] / width_all * inv_row * inv_row
    inv_col = column(inv_row)
    cpl_col = column(cpl_row)

    for h in range(heads):
        grad = inv_col * (gain[h:h + 1, :] * og[h] - att[h] * cpl_col)
        ags[h] = grad
        from_start = jnp.where(lab == first[:, 0:1], jnp.exp(row(h)), 0.0)
        put(own_b, h, mm(split(q[h].T * from_start), split(grad), NN))
        x_b(h).start()

    def local_backward(h):
        grad = split(ags[h])
        gw = wth[h] * mm(grad, split(v[h]), NT)
        p_last = parts(pair_f, h)[2]
        label = even * parts(a_f, h)[2] + odd * p_last
        from_prior = column(jnp.where(lab == label, jnp.exp(row(h)), 0.0))
        dq[h] = mm(split(gw), split(k[h]), NN) + from_prior * mm(grad, split(prior[h]), NT)
        dk[h] = mm(split(gw.T), split(q[h]), NN)
        dv[h] = mm(split(wgt[h].T), grad, NN)

    def merge_backward(h):
        x_b(h).wait_recv()
        p_pass, p_first, p_last = parts(pair_b, h)
        o_pass = passing(h)
        w_even = jnp.where((last == p_first) & (first == last), o_pass, 0.0)
        w_odd = jnp.where((p_last == first) & (p_first == p_last), p_pass, 0.0)
        c_own = even + odd * w_odd
        c_pair = odd + even * w_even
        w_b[h, 0:width, :] = c_own * own_b[h, 0:width, :] + c_pair * pair_b[h, 0:width, :]
        w_b[h, width:width + 8, :] = meta(
            o_pass * p_pass, even * first + odd * p_first, odd * last + even * p_last)

        @pl.when(has_up)
        def _():
            d_a(h).start()

    def relay_backward(h):
        @pl.when(has_down)
        def _():
            d_a(h).wait_recv()

        @pl.when(has_up & has_down)
        def _():
            d_b(h).start()

    def finish_backward(h):
        @pl.when(s < n - 4)
        def _():
            d_b(h).wait_recv()

        a_pass, a_first, a_last = parts(a_b, h)
        b_first = parts(b_b, h)[1]
        p_pass, p_first, p_last = parts(pair_b, h)
        join = jnp.where((a_last == b_first) & (a_first == a_last), a_pass, 0.0)
        step = jnp.where((p_last == a_first) & (p_first == p_last), p_pass, 0.0)
        base = a_b[h, 0:width, :] + join * b_b[h, 0:width, :]
        state = split((odd + even * step) * base + even * pair_b[h, 0:width, :])
        label = odd * a_first + even * p_first
        to_next = column(jnp.where(lab == label, jnp.exp(total(h) - row(h)), 0.0))
        dk[h] = dk[h] + to_next * mm(split(v[h]), state, NT)
        dv[h] = dv[h] + to_next * mm(split(k[h]), state, NN)

    for h in range(half):
        local_backward(h)
    for h in range(heads):
        merge_backward(h)
    for h in range(half, heads):
        local_backward(h)
    for h in range(heads):
        relay_backward(h)
    for h in range(heads):
        finish_backward(h)

    for j in range(1, hs):
        peer(j).wait_send()
    for h in range(heads):
        x_f(h).wait_send()
        x_b(h).wait_send()

        @pl.when(has_down)
        def _():
            c_a(h).wait_send()

        @pl.when(has_up)
        def _():
            d_a(h).wait_send()

        @pl.when(has_up & has_down)
        def _():
            c_b(h).wait_send()
            d_b(h).wait_send()


def per_device(queries, keys, values, out_grad, norm_gain, log_decay, doc_ids):
    n, hs = lax.axis_size("seq"), lax.axis_size("head")
    heads, rows, width = queries.shape
    whole = pl.BlockSpec(memory_space=pltpu.VMEM)
    state = pltpu.VMEM((heads, width + 8, width), F32)
    square = pltpu.VMEM((heads, rows, width), F32)
    scores = pltpu.VMEM((heads, rows, rows), F32)
    out = jax.ShapeDtypeStruct(queries.shape, F32)
    return pl.pallas_call(
        functools.partial(body, n, hs),
        out_shape=(out, out, out),
        in_specs=[pl.BlockSpec(memory_space=pltpu.MemorySpace.HBM)] * 7,
        out_specs=(whole, whole, whole),
        scratch_shapes=[square] * 4 + [
            pltpu.VMEM(norm_gain.shape, F32), pltpu.VMEM(log_decay.shape, F32),
            pltpu.VMEM((1, rows), jnp.int32), pltpu.SemaphoreType.DMA((7,)),
        ] + [state] * 10 + [
            square, scores, scores, pltpu.VMEM((heads, width, width), F32), square,
            pltpu.VMEM((hs, 8, rows), F32),
            pltpu.SemaphoreType.DMA((6, heads)), pltpu.SemaphoreType.DMA((6, heads)),
            pltpu.SemaphoreType.DMA((hs,)), pltpu.SemaphoreType.DMA((hs,)),
        ],
        compiler_params=pltpu.CompilerParams(
            collective_id=0, has_side_effects=True, vmem_limit_bytes=32 * 1024 * 1024),
    )(*[pltpu.with_memory_space_constraint(x, pltpu.MemorySpace.HBM) for x in
        (queries, keys, values, out_grad, norm_gain, log_decay, doc_ids[None, :])])


def solution(mesh):
    in_specs = (
        P("head", "seq", None),
        P("head", "seq", None),
        P("head", "seq", None),
        P("head", "seq", None),
        P("head", None),
        P("head", "seq"),
        P("seq"),
    )
    out_specs = (P("head", "seq", None), P("head", "seq", None), P("head", "seq", None))
    return jax.shard_map(
        per_device, mesh=mesh, in_specs=in_specs, out_specs=out_specs, check_vma=False
    )
```

```python
import functools
import jax
import jax.numpy as jnp
from jax import lax
from jax.experimental import pallas as pl
from jax.experimental.pallas import tpu as pltpu
from jax.sharding import PartitionSpec as P

EPSILON = 1e-06
F32 = jnp.float32
NN = (((1,), (0,)), ((), ()))
NT = (((1,), (1,)), ((), ()))
MESH = pl.DeviceIdType.MESH


def split(x):
    hi = x.astype(jnp.bfloat16)
    lo = (x - hi.astype(F32)).astype(jnp.bfloat16)
    return hi, lo


def mm(a, b, dims):
    left = jnp.concatenate([a[0], a[1], a[0]], axis=1)
    right = jnp.concatenate([b[0], b[0], b[1]], axis=dims[0][1][0])
    return lax.dot_general(left, right, dims, preferred_element_type=F32)


def body(n, hs, q_in, k_in, v_in, og_in, gain_in, ld_in, doc_in, dq, dk, dv,
         q, k, v, og, gain, ld, doc, in_sem,
         own_f, pair_f, w_f, a_f, b_f, own_b, pair_b, w_b, a_b, b_b,
         att, wgt, wth, prior, ags, tot, send, recv, psend, precv):
    heads, rows, width = q.shape
    order = ((ld_in, ld), (doc_in, doc), (k_in, k), (v_in, v), (q_in, q), (og_in, og), (gain_in, gain))
    loads = [pltpu.make_async_copy(a, b, in_sem.at[i]) for i, (a, b) in enumerate(order)]
    for load in loads:
        load.start()
    s = lax.axis_index("seq")
    hd = lax.axis_index("head")
    odd_i = lax.rem(s, 2)
    partner = s + 1 - 2 * odd_i
    odd = odd_i.astype(F32)
    even = 1.0 - odd
    has_up = s >= 2
    has_down = s < n - 2

    barrier = pltpu.get_barrier_semaphore()
    pl.semaphore_signal(barrier, inc=1, device_id={"seq": partner}, device_id_type=MESH)
    for j in range(1, hs):
        pl.semaphore_signal(barrier, inc=1, device_id={"head": lax.rem(hd + j, hs)}, device_id_type=MESH)

    @pl.when(has_up)
    def _():
        pl.semaphore_signal(barrier, inc=1, device_id={"seq": s - 2}, device_id_type=MESH)

    @pl.when(has_down)
    def _():
        pl.semaphore_signal(barrier, inc=1, device_id={"seq": s + 2}, device_id_type=MESH)

    def copy(kind, h, src, dst, to):
        return pltpu.make_async_remote_copy(
            src_ref=src.at[h], dst_ref=dst.at[h], send_sem=send.at[kind, h],
            recv_sem=recv.at[kind, h], device_id={"seq": to}, device_id_type=MESH)

    def x_f(h):
        return copy(0, h, own_f, pair_f, partner)

    def c_a(h):
        return copy(1, h, w_f, a_f, s + 2)

    def c_b(h):
        return copy(2, h, a_f, b_f, s + 2)

    def x_b(h):
        return copy(3, h, own_b, pair_b, partner)

    def d_a(h):
        return copy(4, h, w_b, a_b, s - 2)

    def d_b(h):
        return copy(5, h, a_b, b_b, s - 2)

    loads[0].wait()
    loads[1].wait()
    ri = lax.broadcasted_iota(jnp.int32, (rows, rows), 0)
    ci = lax.broadcasted_iota(jnp.int32, (rows, rows), 1)
    tri = jnp.where(ri <= ci, 1.0, 0.0)
    cum = lax.dot_general(ld[...], tri, NN, precision=lax.Precision.HIGHEST, preferred_element_type=F32)
    lab = doc[...].astype(F32) + 1.0
    first = jnp.broadcast_to(lab[:, 0:1], (1, width))
    last = jnp.broadcast_to(lab[:, rows - 1:rows], (1, width))
    mi = lax.broadcasted_iota(jnp.int32, (8, width), 0)

    def meta(passing, first_row, last_row):
        return jnp.where(mi == 0, passing, jnp.where(mi == 1, first_row, last_row))

    def parts(buf, h):
        return (buf[h, rows:rows + 1, :], buf[h, rows + 1:rows + 2, :], buf[h, rows + 2:rows + 3, :])

    def row(h):
        return cum[h:h + 1, :]

    def total(h):
        return cum[h:h + 1, rows - 1:rows]

    def passing(h):
        return jnp.broadcast_to(jnp.exp(total(h)), (1, width))

    def column(r):
        return jnp.broadcast_to(r, (width, r.shape[1])).T

    def put(buf, h, state):
        buf[h, 0:width, :] = state
        buf[h, width:width + 8, :] = meta(passing(h), first, last)

    loads[2].wait()
    loads[3].wait()
    for h in range(heads):
        tail = jnp.where(lab == last[:, 0:1], jnp.exp(total(h) - row(h)), 0.0)
        put(own_f, h, mm(split(k[h].T * tail), split(v[h]), NN))
        if h == 0:
            count = hs + has_up.astype(jnp.int32) + has_down.astype(jnp.int32)
            pl.semaphore_wait(barrier, count)
        x_f(h).start()

    @pl.when(s < 2)
    def _():
        a_f[...] = jnp.zeros_like(a_f)

    @pl.when(s < 4)
    def _():
        b_f[...] = jnp.zeros_like(b_f)

    @pl.when(s >= n - 2)
    def _():
        a_b[...] = jnp.zeros_like(a_b)

    @pl.when(s >= n - 4)
    def _():
        b_b[...] = jnp.zeros_like(b_b)

    lab_col = column(lab)
    allowed = (lab_col == lab) & (ri >= ci)

    def local_forward(h):
        spread = column(row(h)) - row(h)
        within = jnp.where(allowed, jnp.exp(jnp.where(allowed, spread, 0.0)), 0.0)
        wth[h] = within
        weighted = within * mm(split(q[h]), split(k[h]), NT)
        wgt[h] = weighted
        att[h] = mm(split(weighted), split(v[h]), NN)

    def merge_forward(h):
        x_f(h).wait_recv()
        p_pass, p_first, p_last = parts(pair_f, h)
        o_pass = passing(h)
        w_even = jnp.where((last == p_first) & (p_first == p_last), p_pass, 0.0)
        w_odd = jnp.where((p_last == first) & (first == last), o_pass, 0.0)
        c_own = odd + even * w_even
        c_pair = even + odd * w_odd
        w_f[h, 0:width, :] = c_own * own_f[h, 0:width, :] + c_pair * pair_f[h, 0:width, :]
        w_f[h, width:width + 8, :] = meta(
            o_pass * p_pass, even * first + odd * p_first, odd * last + even * p_last)

        @pl.when(has_down)
        def _():
            c_a(h).start()

    def relay_forward(h):
        @pl.when(has_up)
        def _():
            c_a(h).wait_recv()

        @pl.when(has_up & has_down)
        def _():
            c_b(h).start()

    def finish_forward(h):
        @pl.when(s >= 4)
        def _():
            c_b(h).wait_recv()

        a_pass, a_first, a_last = parts(a_f, h)
        b_last = parts(b_f, h)[2]
        p_pass, p_first, p_last = parts(pair_f, h)
        join = jnp.where((b_last == a_first) & (a_first == a_last), a_pass, 0.0)
        step = jnp.where((a_last == p_first) & (p_first == p_last), p_pass, 0.0)
        base = a_f[h, 0:width, :] + join * b_f[h, 0:width, :]
        state = (even + odd * step) * base + odd * pair_f[h, 0:width, :]
        prior[h] = state
        label = even * a_last + odd * p_last
        from_prior = column(jnp.where(lab == label, jnp.exp(row(h)), 0.0))
        attended = att[h] + from_prior * mm(split(q[h]), split(state), NN)
        att[h] = attended
        scaled = gain[h:h + 1, :] * og[h]
        return attended * attended, scaled * attended

    half = heads // 2
    for load in loads[4:]:
        load.wait()
    for h in range(half):
        local_forward(h)
    for h in range(heads):
        merge_forward(h)
        if h % 2 == 0 and half + h // 2 < heads:
            local_forward(half + h // 2)
        if h >= 2:
            relay_forward(h - 2)
    for h in range(max(heads - 2, 0), heads):
        relay_forward(h)
    squares, inner = None, None
    for h in range(heads):
        one, two = finish_forward(h)
        squares = one if h == 0 else squares + one
        inner = two if h == 0 else inner + two
    sum_sq = jnp.sum(squares.T, axis=0, keepdims=True)
    sum_in = jnp.sum(inner.T, axis=0, keepdims=True)
    tot[0] = jnp.where(mi == 0, sum_sq, sum_in)

    def peer(j):
        return pltpu.make_async_remote_copy(
            src_ref=tot.at[0], dst_ref=tot.at[j], send_sem=psend.at[j], recv_sem=precv.at[j],
            device_id={"head": lax.rem(hd + j, hs)}, device_id_type=MESH)

    for j in range(1, hs):
        peer(j).start()
    for j in range(1, hs):
        peer(j).wait_recv()
    totals = tot[0]
    for j in range(1, hs):
        totals = totals + tot[j]
    width_all = heads * width * hs
    inv_row = lax.rsqrt(totals[0:1, :] / width_all + EPSILON)
    cpl_row = totals[1:2, :] / width_all * inv_row * inv_row
    inv_col = column(inv_row)
    cpl_col = column(cpl_row)

    for h in range(heads):
        grad = inv_col * (gain[h:h + 1, :] * og[h] - att[h] * cpl_col)
        ags[h] = grad
        from_start = jnp.where(lab == first[:, 0:1], jnp.exp(row(h)), 0.0)
        put(own_b, h, mm(split(q[h].T * from_start), split(grad), NN))
        x_b(h).start()

    def local_backward(h):
        grad = split(ags[h])
        gw = wth[h] * mm(grad, split(v[h]), NT)
        p_last = parts(pair_f, h)[2]
        label = even * parts(a_f, h)[2] + odd * p_last
        from_prior = column(jnp.where(lab == label, jnp.exp(row(h)), 0.0))
        dq[h] = mm(split(gw), split(k[h]), NN) + from_prior * mm(grad, split(prior[h]), NT)
        dk[h] = mm(split(gw.T), split(q[h]), NN)
        dv[h] = mm(split(wgt[h].T), grad, NN)

    def merge_backward(h):
        x_b(h).wait_recv()
        p_pass, p_first, p_last = parts(pair_b, h)
        o_pass = passing(h)
        w_even = jnp.where((last == p_first) & (first == last), o_pass, 0.0)
        w_odd = jnp.where((p_last == first) & (p_first == p_last), p_pass, 0.0)
        c_own = even + odd * w_odd
        c_pair = odd + even * w_even
        w_b[h, 0:width, :] = c_own * own_b[h, 0:width, :] + c_pair * pair_b[h, 0:width, :]
        w_b[h, width:width + 8, :] = meta(
            o_pass * p_pass, even * first + odd * p_first, odd * last + even * p_last)

        @pl.when(has_up)
        def _():
            d_a(h).start()

    def relay_backward(h):
        @pl.when(has_down)
        def _():
            d_a(h).wait_recv()

        @pl.when(has_up & has_down)
        def _():
            d_b(h).start()

    def finish_backward(h):
        @pl.when(s < n - 4)
        def _():
            d_b(h).wait_recv()

        a_pass, a_first, a_last = parts(a_b, h)
        b_first = parts(b_b, h)[1]
        p_pass, p_first, p_last = parts(pair_b, h)
        join = jnp.where((a_last == b_first) & (a_first == a_last), a_pass, 0.0)
        step = jnp.where((p_last == a_first) & (p_first == p_last), p_pass, 0.0)
        base = a_b[h, 0:width, :] + join * b_b[h, 0:width, :]
        state = split((odd + even * step) * base + even * pair_b[h, 0:width, :])
        label = odd * a_first + even * p_first
        to_next = column(jnp.where(lab == label, jnp.exp(total(h) - row(h)), 0.0))
        dk[h] = dk[h] + to_next * mm(split(v[h]), state, NT)
        dv[h] = dv[h] + to_next * mm(split(k[h]), state, NN)

    for h in range(half):
        local_backward(h)
    for h in range(heads):
        merge_backward(h)
        if h % 2 == 0 and half + h // 2 < heads:
            local_backward(half + h // 2)
        if h >= 2:
            relay_backward(h - 2)
    for h in range(max(heads - 2, 0), heads):
        relay_backward(h)
    for h in range(heads):
        finish_backward(h)

    for j in range(1, hs):
        peer(j).wait_send()
    for h in range(heads):
        x_f(h).wait_send()
        x_b(h).wait_send()

        @pl.when(has_down)
        def _():
            c_a(h).wait_send()

        @pl.when(has_up)
        def _():
            d_a(h).wait_send()

        @pl.when(has_up & has_down)
        def _():
            c_b(h).wait_send()
            d_b(h).wait_send()


def per_device(queries, keys, values, out_grad, norm_gain, log_decay, doc_ids):
    n, hs = lax.axis_size("seq"), lax.axis_size("head")
    heads, rows, width = queries.shape
    whole = pl.BlockSpec(memory_space=pltpu.VMEM)
    state = pltpu.VMEM((heads, width + 8, width), F32)
    square = pltpu.VMEM((heads, rows, width), F32)
    scores = pltpu.VMEM((heads, rows, rows), F32)
    out = jax.ShapeDtypeStruct(queries.shape, F32)
    return pl.pallas_call(
        functools.partial(body, n, hs),
        out_shape=(out, out, out),
        in_specs=[pl.BlockSpec(memory_space=pltpu.MemorySpace.HBM)] * 7,
        out_specs=(whole, whole, whole),
        scratch_shapes=[square] * 4 + [
            pltpu.VMEM(norm_gain.shape, F32), pltpu.VMEM(log_decay.shape, F32),
            pltpu.VMEM((1, rows), jnp.int32), pltpu.SemaphoreType.DMA((7,)),
        ] + [state] * 10 + [
            square, scores, scores, pltpu.VMEM((heads, width, width), F32), square,
            pltpu.VMEM((hs, 8, rows), F32),
            pltpu.SemaphoreType.DMA((6, heads)), pltpu.SemaphoreType.DMA((6, heads)),
            pltpu.SemaphoreType.DMA((hs,)), pltpu.SemaphoreType.DMA((hs,)),
        ],
        compiler_params=pltpu.CompilerParams(
            collective_id=0, has_side_effects=True, vmem_limit_bytes=32 * 1024 * 1024),
    )(*[pltpu.with_memory_space_constraint(x, pltpu.MemorySpace.HBM) for x in
        (queries, keys, values, out_grad, norm_gain, log_decay, doc_ids[None, :])])


def solution(mesh):
    in_specs = (
        P("head", "seq", None),
        P("head", "seq", None),
        P("head", "seq", None),
        P("head", "seq", None),
        P("head", None),
        P("head", "seq"),
        P("seq"),
    )
    out_specs = (P("head", "seq", None), P("head", "seq", None), P("head", "seq", None))
    return jax.shard_map(
        per_device, mesh=mesh, in_specs=in_specs, out_specs=out_specs, check_vma=False
    )
```
